32 devices in a mesh: parts: 1, var: 8 (over z, core), patch: 4 (over y, x).
Axes of the slice: x: 2, y: 2, z: 4, core: 2. Of those that a mesh axis runs over, the one named last changes fastest.
Arguments:
- tokens: bfloat16 [256, 24, 768], P('patch', ('parts', 'var')), may hold values from -6 to 6
- patch_mask: int32 [256, 24], P('patch', ('parts', 'var')), may hold values 0 or 1
- group_ids: int32 [24], P('parts'), may hold values from 0 to 7, never falling along the last dimension, each value on 1 to 6 neighbouring positions
- time_gain: float32 [768], replicated, may hold values from 0.1 to 1.9
- time_qkv: bfloat16 [768, 3, 768], P(None, None, 'patch'), may hold values from -0.21875 to 0.21875
- time_out: bfloat16 [768, 768], P('patch'), may hold values from -0.21875 to 0.21875
- space_gain: float32 [768], replicated, may hold values from 0.1 to 1.9
- space_qkv: bfloat16 [768, 3, 768], P(None, None, 'patch'), may hold values from -0.21875 to 0.21875
- space_out: bfloat16 [768, 768], P('patch'), may hold values from -0.21875 to 0.21875
Outputs:
- panel_out: bfloat16 [256, 24, 768], P('patch', ('parts', 'var'))
The draws below stay inside these ranges and needn't reach their ends.
Inputs may be any that keep to these rules, and one draw needn't show every extreme that they name: group_ids never falls along the variates; each group is a run of 1 to 6 consecutive variates.
All inputs are finite; a program needn't handle non-finite values. No bound on the sum of `patch_mask` on one device may be relied on, other than what follows from the above.
Results may differ from the reference program's by a relative error of at most 0.017.
Values may be sent and summed in bfloat16 or wider, within the bound.
A program may use at most 64 MiB of HBM per device.

```python
import math
import jax
import jax.numpy as jnp
import numpy as np
from jax import lax

D = 768
HEADS = 12
HD = 64
VAR_DEV = 3
V = 24
P_SIZE = 256
GMAX = 6
GROUPS = 8
N_PATCH = 4


def plant(result, key, low, top_value):
    extent = result.shape
    place = [jax.random.randint(jax.random.fold_in(key, axis), (), 0, extent[axis]) for axis in range(len(extent))]
    result = result.at[tuple(place)].set(low)
    longest = extent.index(max(extent))
    place[longest] = (place[longest] + 1) % extent[longest]
    return result.at[tuple(place)].set(top_value)


def block_levels(key, shape, cuts, least, largest):
    factor_of = 1.0
    for dim, blocks in cuts:
        draws = jax.random.uniform(jax.random.fold_in(jax.random.fold_in(key, 6), dim), (blocks,), jnp.float32, least / len(cuts), largest / len(cuts))
        factor_of = factor_of * jnp.repeat(jnp.exp(draws), shape[dim] // blocks).reshape((-1,) + (1,) * (len(shape) - 1 - dim))
    return factor_of


def split_up(number_of, total, limit, skew):
    weights = [(1 << 20) // math.isqrt(grade ** skew) + 1 for grade in range(2, number_of + 1)]
    surplus, holding = total - limit - (number_of - 1), [1] * (number_of - 1)
    while surplus > 0:
        movable = [i for i in range(number_of - 1) if holding[i] < limit]
        mass, remaining = sum([weights[i] for i in movable]), surplus
        for i in movable:
            more = min(limit - holding[i], max(1, remaining * weights[i] // mass), surplus)
            holding[i] = holding[i] + more
            surplus = surplus - more
    return np.array([limit] + holding)


def uneven(own_key, count, total, limit, skew):
    if count == 2:
        one = jax.random.randint(own_key, (), max(1, total - limit), min(limit, total - 1) + 1)
        return jnp.stack([one, total - one])
    lengths = jnp.asarray(split_up(count, total, limit, skew), jnp.int32)
    twos = (count - 1) // 2
    source_of, receiver = lengths[1:1 + 2 * twos:2], lengths[2:2 + 2 * twos:2]
    slack = jnp.minimum(source_of - 1, limit - receiver)
    shifted = jax.random.randint(jax.random.fold_in(own_key, 1), (twos,), 0, 1 << 20) % (slack + 1)
    lengths = lengths.at[1:1 + 2 * twos:2].set(source_of - shifted).at[2:2 + 2 * twos:2].set(receiver + shifted)
    return lengths[jax.random.permutation(jax.random.fold_in(own_key, 2), count)]


def normal_values(key, extent, deviation, limit, cuts=(), kind=jnp.bfloat16):
    level = block_levels(key, extent, cuts, -0.22, 0.18) if cuts else 1.0
    array = jax.random.normal(key, extent, jnp.float32) * deviation * level
    return jnp.minimum(jnp.maximum(array, -limit), limit).astype(kind)


def setup_inputs(seed: int = 0, part: int = 0) -> dict:
    keys = jax.random.split(jax.random.key(seed), 10)
    part_keys = jax.random.split(jax.random.fold_in(keys[9], part), 10)
    tokens = normal_values(part_keys[0], (P_SIZE, V, D), 1.0, 6.0, ((0, 4), (1, 8)))
    patch_mask = plant((jax.random.randint(part_keys[1], (P_SIZE, V), 0, 4) < 3).astype(jnp.int32), jax.random.fold_in(part_keys[1], 1), 0, 1)
    group_ids = jnp.searchsorted(jnp.cumsum(uneven(part_keys[2], GROUPS, V, GMAX, 2)), jnp.arange(V), side="right").astype(jnp.int32)
    time_gain = jnp.clip(1.0 + 0.18 * jax.random.normal(keys[3], (D,), jnp.float32), 0.1, 1.9)
    time_qkv = normal_values(keys[4], (D, 3, D), D ** -0.5, 0.21875, ((2, 4),))
    time_out = normal_values(keys[5], (D, D), D ** -0.5, 0.21875, ((0, 4),))
    space_gain = jnp.clip(1.0 + 0.18 * jax.random.normal(keys[6], (D,), jnp.float32), 0.1, 1.9)
    space_qkv = normal_values(keys[7], (D, 3, D), D ** -0.5, 0.21875, ((2, 4),))
    space_out = normal_values(keys[8], (D, D), D ** -0.5, 0.21875, ((0, 4),))
    return {"tokens": tokens, "patch_mask": patch_mask, "group_ids": group_ids, "time_gain": time_gain, "time_qkv": time_qkv, "time_out": time_out, "space_gain": space_gain, "space_qkv": space_qkv, "space_out": space_out}


epsilon = 1e-06

def norm_rows(block_rows, gain):
    floats = block_rows.astype(jnp.float32)
    scaled = floats * lax.rsqrt(lax.optimization_barrier(jnp.mean(floats * floats, axis=-1, keepdims=True)) + epsilon)
    return (scaled * gain.astype(jnp.float32)).astype(jnp.bfloat16)

def project(normed, weight):
    return jnp.einsum('pvd,dtk->pvtk', normed.astype(jnp.float32), weight.astype(jnp.float32)).astype(jnp.bfloat16)

def soft_weights(scores, allowed):
    masked = jnp.where(allowed, scores, -jnp.inf)
    highest = lax.optimization_barrier(jnp.max(masked, axis=-1, keepdims=True))
    raised = jnp.exp(masked - highest)
    return (raised / lax.optimization_barrier(jnp.sum(raised, axis=-1, keepdims=True))).astype(jnp.bfloat16)

def head_sum(attended, weight):
    group_width = D // N_PATCH
    lead_shape = attended.shape[:-1]
    flat = attended.reshape(-1, D)
    summed = jnp.zeros((flat.shape[0], D), jnp.float32)
    for group in range(N_PATCH):
        part = jnp.dot(flat[:, group * group_width:(group + 1) * group_width], weight[group * group_width:(group + 1) * group_width], preferred_element_type=jnp.float32)
        part = lax.optimization_barrier(part.astype(jnp.bfloat16))
        summed = summed + part.astype(jnp.float32)
    return summed.reshape(lead_shape + (D,))

def time_block(block_rows, block_mask, gain, weight, out_weight):
    patch_count, var_count = (block_rows.shape[0], block_rows.shape[1])
    projected = project(norm_rows(block_rows, gain), weight)
    queries = projected[:, :, 0].reshape(patch_count, var_count, HEADS, HD).astype(jnp.float32)
    key_rows = projected[:, :, 1].reshape(patch_count, var_count, HEADS, HD).astype(jnp.float32)
    value_rows = projected[:, :, 2].reshape(patch_count, var_count, HEADS, HD).astype(jnp.float32)
    scores = jnp.einsum('qvhe,kvhe->vhqk', queries, key_rows) * HD ** (-0.5)
    query_pos = jnp.arange(patch_count)[:, None]
    key_pos = jnp.arange(patch_count)[None, :]
    observed = (block_mask.T > 0)[:, None, None, :]
    allowed = (key_pos <= query_pos)[None, None] & (observed | (key_pos == query_pos)[None, None])
    weights = soft_weights(scores, allowed)
    attended = jnp.einsum('vhqk,kvhe->qvhe', weights.astype(jnp.float32), value_rows).astype(jnp.bfloat16)
    attended = attended.reshape(patch_count, var_count, D)
    mixed = head_sum(attended, out_weight)
    return (block_rows.astype(jnp.float32) + mixed).astype(jnp.bfloat16)

def space_block(block_rows, group_ids, gain, weight, out_weight):
    patch_count, var_count = (block_rows.shape[0], block_rows.shape[1])
    projected = project(norm_rows(block_rows, gain), weight)
    queries = projected[:, :, 0].reshape(patch_count, var_count, HEADS, HD).astype(jnp.float32)
    key_rows = projected[:, :, 1].reshape(patch_count, var_count, HEADS, HD).astype(jnp.float32)
    value_rows = projected[:, :, 2].reshape(patch_count, var_count, HEADS, HD).astype(jnp.float32)
    scores = jnp.einsum('pqhe,pkhe->phqk', queries, key_rows) * HD ** (-0.5)
    allowed = (group_ids[:, None] == group_ids[None, :])[None, None]
    weights = soft_weights(scores, allowed)
    attended = jnp.einsum('phqk,pkhe->pqhe', weights.astype(jnp.float32), value_rows).astype(jnp.bfloat16)
    attended = attended.reshape(patch_count, var_count, D)
    mixed = head_sum(attended, out_weight)
    return (block_rows.astype(jnp.float32) + mixed).astype(jnp.bfloat16)

def reference(tokens, patch_mask, group_ids, time_gain, time_qkv, time_out, space_gain, space_qkv, space_out):
    block_count = V // VAR_DEV

    def time_step(block):
        start = (block * VAR_DEV).astype(jnp.int32)
        rows_in = lax.dynamic_slice_in_dim(tokens, start, VAR_DEV, 1)
        mask_in = lax.dynamic_slice_in_dim(patch_mask, start, VAR_DEV, 1)
        return time_block(rows_in, mask_in, time_gain, time_qkv, time_out)
    middle = lax.map(time_step, jnp.arange(block_count, dtype=jnp.int32))
    middle = jnp.transpose(middle, (1, 0, 2, 3)).reshape(P_SIZE, V, D)
    patch_blocks = P_SIZE // N_PATCH

    def space_step(block):
        start = (block * N_PATCH).astype(jnp.int32)
        rows_in = lax.dynamic_slice_in_dim(middle, start, N_PATCH, 0)
        return space_block(rows_in, group_ids, space_gain, space_qkv, space_out)
    final = lax.map(space_step, jnp.arange(patch_blocks, dtype=jnp.int32))
    return final.reshape(P_SIZE, V, D)
```

```python
import functools

import jax
import jax.numpy as jnp
from jax import lax
from jax.experimental import pallas as pl
from jax.experimental.pallas import tpu as pltpu
from jax.sharding import PartitionSpec as P

HD = 64
REACH = 5
EPS = 1e-06
MESH = pl.DeviceIdType.MESH
F32 = jnp.float32
BF16 = jnp.bfloat16


def norm_rows(rows, gain):
    floats = rows.astype(F32)
    scaled = floats * lax.rsqrt(jnp.mean(floats * floats, axis=-1, keepdims=True) + EPS)
    return (scaled * gain).astype(BF16)


def dot(a, b):
    return jnp.dot(a, b, preferred_element_type=F32)


def kernel(
    n, nvar, tok, marks, gids, tgain, sgain, wt_in, wot_in, wqs_in, wos_in,
    out, gx, mk, wt, wot, wqs, wos, att, ratt, mid, sw, kvb, qb, prod, sc, pb,
    local_sem, tok_s, tok_r, mk_s, mk_r, w_s, w_r, att_s, att_r, win_s, win_r,
):
    me = lax.axis_index("patch")
    var = lax.axis_index("var")
    nv, pp, dm = tok.shape
    hw = wot_in.shape[0]
    heads = hw // HD
    sib = var + 1 - 2 * (var % 2)
    par = var + 2 - 4 * ((var // 2) % 2)
    quarter = var % 4
    sib_q = sib % 4
    par_q = par % 4
    nbrs = (1, -1, 2, -2)

    def exists(k):
        return (var + k >= 0) & (var + k < nvar)

    def peer(d):
        return (me + d) % n

    def source(d):
        return (me + n - d) % n

    barrier = pltpu.get_barrier_semaphore()
    count = n - 1 + 2
    for d in range(1, n):
        pl.semaphore_signal(barrier, inc=1, device_id={"patch": peer(d)}, device_id_type=MESH)
    for other in (sib, par):
        pl.semaphore_signal(barrier, inc=1, device_id={"var": other}, device_id_type=MESH)
    for k in nbrs:
        @pl.when(exists(k))
        def _():
            pl.semaphore_signal(barrier, inc=1, device_id={"var": var + k}, device_id_type=MESH)
        count = count + exists(k).astype(jnp.int32)
    pl.semaphore_wait(barrier, count)

    sends = []

    def remote(src, dst, ssem, rsem, **where):
        c = pltpu.make_async_remote_copy(
            src_ref=src, dst_ref=dst, send_sem=ssem, recv_sem=rsem, device_id=where, device_id_type=MESH
        )
        return c

    def launch(*a, **k):
        c = remote(*a, **k)
        c.start()
        sends.append(c)
        return c

    mine = pl.ds(pl.multiple_of(me * pp, pp), pp)
    tok_c, mk_c = [], []
    for d in range(1, n):
        mk_c.append(launch(marks, mk.at[me], mk_s.at[d], mk_r.at[d], patch=peer(d)))
    for d in (1, 3, 2) if n == 4 else range(1, n):
        tok_c.append(launch(tok, gx.at[:, mine, :], tok_s.at[d], tok_r.at[d], patch=peer(d)))

    arrays = ((wot_in, wot), (wqs_in, wqs), (wos_in, wos))

    def part(buf, shard, q):
        rows = buf.shape[1] // 4
        return buf.at[shard, pl.ds(pl.multiple_of(q * rows, rows), rows), :]

    first = {}
    for a, (src, dst) in enumerate(arrays):
        rows = src.shape[0] // 4
        for d in range(1, n):
            first[a, d] = launch(
                src.at[pl.ds(pl.multiple_of(quarter * rows, rows), rows), :], part(dst, me, quarter),
                w_s.at[0, a, d], w_r.at[0, a, d], patch=peer(d),
            )
    second, third, fourth = {}, {}, {}

    def forward(a):
        buf = arrays[a][1]
        for d in range(1, n):
            first[a, d].wait_recv()
            piece = part(buf, source(d), quarter)
            third[a, d] = launch(piece, piece, w_s.at[2, a, d], w_r.at[2, a, d], var=par)
            second[a, d] = launch(piece, piece, w_s.at[1, a, d], w_r.at[1, a, d], var=sib)

    def relay(a):
        buf = arrays[a][1]
        for d in range(1, n):
            third[a, d].wait_recv()
            piece = part(buf, source(d), par_q)
            fourth[a, d] = launch(piece, piece, w_s.at[3, a, d], w_r.at[3, a, d], var=sib)

    def arrived(a):
        for d in range(1, n):
            second[a, d].wait_recv()
            fourth[a, d].wait_recv()

    own = [
        pltpu.make_async_copy(wt_in, wt, local_sem.at[0]),
        pltpu.make_async_copy(wot_in, wot.at[me], local_sem.at[1]),
        pltpu.make_async_copy(wqs_in, wqs.at[me], local_sem.at[2]),
        pltpu.make_async_copy(wos_in, wos.at[me], local_sem.at[3]),
    ]
    for c in own:
        c.start()

    for k in nbrs:
        lo = {1: 9, -1: 3, 2: 12, -2: 1}[k]
        num = nv if abs(k) == 1 else nv - 1

        @pl.when(jnp.logical_not(exists(k)))
        def _():
            sw[lo:lo + num] = jnp.zeros((num, pp, dm), BF16)

    gx[:, mine, :] = tok[...]
    mk[me] = marks[...]
    own[0].wait()
    for c in mk_c:
        c.wait_recv()
    for c in tok_c:
        c.wait_recv()

    full = n * pp
    seen = mk[0]
    for s in range(1, n):
        seen = seen + mk[s]
    qi = lax.broadcasted_iota(jnp.int32, (full, full), 0)
    ki = lax.broadcasted_iota(jnp.int32, (full, full), 1)
    att_c = []
    for v in range(nv):
        normed = norm_rows(gx[v], tgain[...])
        proj = dot(normed, wt[...]).astype(BF16)
        allowed = ((ki < qi) & (seen[v:v + 1, :] > 0.5)) | (ki == qi)
        outs = []
        for h in range(heads):
            q = proj[:, h * HD:(h + 1) * HD]
            k = proj[:, hw + h * HD:hw + (h + 1) * HD]
            val = proj[:, 2 * hw + h * HD:2 * hw + (h + 1) * HD]
            s = lax.dot_general(q, k, (((1,), (1,)), ((), ())), preferred_element_type=F32) * HD ** (-0.5)
            s = jnp.where(allowed, s, -jnp.inf)
            e = jnp.exp(s - jnp.max(s, axis=-1, keepdims=True))
            w = (e / jnp.sum(e, axis=-1, keepdims=True)).astype(BF16)
            outs.append(dot(w, val).astype(BF16))
        att[v] = jnp.concatenate(outs, axis=1)
        for d in range(1, n):
            there = pl.ds(pl.multiple_of(peer(d) * pp, pp), pp)
            att_c.append(launch(att.at[v, there, :], ratt.at[me, v], att_s.at[v, d], att_r.at[v, d], patch=peer(d)))
        ratt[me, v] = att[v, mine, :]
        if v == 0:
            forward(0)
        if v == 1:
            forward(1)
    relay(0)
    own[1].wait()
    arrived(0)
    for c in att_c:
        c.wait_recv()

    rows = nv * pp
    mix = jnp.zeros((rows, dm), F32)
    for s in range(n):
        mix = mix + dot(ratt[s].reshape(rows, hw), wot[s]).astype(BF16).astype(F32)
    middle = (tok[...].reshape(rows, dm).astype(F32) + mix).astype(BF16)
    mid[...] = middle
    sw[6:6 + nv] = norm_rows(middle, sgain[...]).reshape(nv, pp, dm)

    def window(k, i):
        src = {1: (6, 9), -1: (6, 9), 2: (7, 9), -2: (6, 8)}[k]
        dst = {1: (3, 6), -1: (9, 12), 2: (1, 3), -2: (12, 14)}[k]
        return remote(sw.at[src[0]:src[1]], sw.at[dst[0]:dst[1]], win_s.at[i], win_r.at[i], var=var + k)

    for i, k in enumerate(nbrs):
        @pl.when(exists(k))
        def _():
            window(k, i).start()

    forward(2)
    relay(1)
    own[2].wait()
    arrived(1)
    for i, k in enumerate(nbrs):
        @pl.when(exists(-k))
        def _():
            window(k, i).wait_recv()

    nkey = 4 + 3 * nv
    pairs = [(u, u + 6 + t) for u in range(nv) for t in range(-REACH, REACH + 1)]
    sc[...] = jnp.zeros_like(sc)

    def scores_of(s, carry):
        qb[...] = dot(sw[6:6 + nv].reshape(rows, dm), wqs[s, :, 2 * hw:]).astype(BF16).reshape(nv, pp, hw)
        kvb[s] = dot(sw[1:1 + nkey].reshape(nkey * pp, dm), wqs[s, :, :2 * hw]).astype(BF16).reshape(nkey, pp, 2 * hw)
        for i, (u, j) in enumerate(pairs):
            prod[i * pp:(i + 1) * pp, :] = (
                qb[u].astype(F32) * kvb[s, j - 1, :, :hw].astype(F32)
            ).astype(BF16)
        lane = lax.broadcasted_iota(jnp.int32, (hw, 128), 0) // HD + heads * s
        col = lax.broadcasted_iota(jnp.int32, (hw, 128), 1)
        sc[...] += dot(prod[...], (lane == col).astype(F32).astype(BF16))
        return carry

    lax.fori_loop(0, n, scores_of, 0)

    total = gids.shape[0]
    local_n = total // nv
    base = (var % local_n) * nv
    for u in range(nv):
        mine_group = gids[base + u]
        slabs = []
        for t in range(-REACH, REACH + 1):
            w = base + u + t
            inside = (w >= 0) & (w < total)
            at = jnp.minimum(jnp.maximum(w, 0), total - 1)
            i = pairs.index((u, u + 6 + t))
            ok = inside & (gids[at] == mine_group)
            slabs.append(jnp.where(ok, sc[i * pp:(i + 1) * pp, :] * HD ** (-0.5), -jnp.inf))
        top = functools.reduce(jnp.maximum, slabs)
        es = [jnp.exp(x - top) for x in slabs]
        den = functools.reduce(lambda a, b: a + b, es)
        for t, e in enumerate(es):
            i = u * (2 * REACH + 1) + t
            pb[i * pp:(i + 1) * pp, :] = (e / den).astype(BF16)

    relay(2)
    own[3].wait()
    arrived(2)

    def mix_of(s, acc):
        lane = lax.broadcasted_iota(jnp.int32, (128, hw), 1) // HD + heads * s
        col = lax.broadcasted_iota(jnp.int32, (128, hw), 0)
        spread = (lane == col).astype(F32).astype(BF16)
        done = []
        for u in range(nv):
            total_u = jnp.zeros((pp, hw), F32)
            lo = u * (2 * REACH + 1)
            wide = dot(pb[lo * pp:(lo + 2 * REACH + 1) * pp, :], spread)
            for t in range(2 * REACH + 1):
                val = kvb[s, u + t, :, hw:].astype(F32)
                total_u = total_u + wide[t * pp:(t + 1) * pp] * val
            done.append(total_u.astype(BF16))
        res = dot(jnp.concatenate(done, axis=0), wos[s]).astype(BF16).astype(F32)
        return acc + res

    mix2 = lax.fori_loop(0, n, mix_of, jnp.zeros((rows, dm), F32))
    out[...] = (mid[...].astype(F32) + mix2).astype(BF16).reshape(nv, pp, dm)

    for c in sends:
        c.wait_send()
    for i, k in enumerate(nbrs):
        @pl.when(exists(k))
        def _():
            window(k, i).wait_send()


def on_device(n, nvar, tokens, patch_mask, group_ids, time_gain, time_qkv, time_out, space_gain, space_qkv, space_out):
    pp, nv, dm = tokens.shape
    hw = time_out.shape[0]
    me = lax.axis_index("patch")
    tok = jnp.transpose(tokens, (1, 0, 2))
    marks = lax.dynamic_update_slice(
        jnp.zeros((8, n * pp), F32), patch_mask.T.astype(F32), (0, me * pp)
    )
    wt = time_qkv.reshape(dm, 3 * hw)
    wqs = jnp.concatenate([space_qkv[:, 1], space_qkv[:, 2], space_qkv[:, 0]], axis=1)
    npair = nv * (2 * REACH + 1)
    vm = pl.BlockSpec(memory_space=pltpu.VMEM)
    anyv = pl.BlockSpec(memory_space=pl.ANY)
    dma = pltpu.SemaphoreType.DMA
    res = pl.pallas_call(
        functools.partial(kernel, n, nvar),
        out_shape=jax.ShapeDtypeStruct((nv, pp, dm), BF16),
        in_specs=[vm, vm, pl.BlockSpec(memory_space=pltpu.SMEM), vm, vm, anyv, anyv, anyv, anyv],
        out_specs=vm,
        scratch_shapes=[
            pltpu.VMEM((nv, n * pp, dm), BF16),
            pltpu.VMEM((n, 8, n * pp), F32),
            pltpu.VMEM((dm, 3 * hw), BF16),
            pltpu.VMEM((n, hw, dm), BF16),
            pltpu.VMEM((n, dm, 3 * hw), BF16),
            pltpu.VMEM((n, hw, dm), BF16),
            pltpu.VMEM((nv, n * pp, hw), BF16),
            pltpu.VMEM((n, nv, pp, hw), BF16),
            pltpu.VMEM((nv * pp, dm), BF16),
            pltpu.VMEM((5 * nv, pp, dm), BF16),
            pltpu.VMEM((n, 4 + 3 * nv, pp, 2 * hw), BF16),
            pltpu.VMEM((nv, pp, hw), BF16),
            pltpu.VMEM((npair * pp, hw), BF16),
            pltpu.VMEM((npair * pp, 128), F32),
            pltpu.VMEM((npair * pp, 128), BF16),
            dma((4,)), dma((n,)), dma((n,)), dma((n,)), dma((n,)),
            dma((4, 3, n)), dma((4, 3, n)), dma((nv, n)), dma((nv, n)), dma((4,)), dma((4,)),
        ],
        compiler_params=pltpu.CompilerParams(
            collective_id=0, has_side_effects=True, vmem_limit_bytes=52 * 2**20
        ),
    )(tok, marks, group_ids, time_gain[None], space_gain[None], wt, time_out, wqs, space_out)
    return jnp.transpose(res, (1, 0, 2))


def solution(mesh):
    in_specs = (
        P("patch", ("parts", "var"), None),
        P("patch", ("parts", "var")),
        P("parts"),
        P(),
        P(None, None, "patch"),
        P("patch", None),
        P(),
        P(None, None, "patch"),
        P("patch", None),
    )
    out_specs = P("patch", ("parts", "var"), None)
    return jax.shard_map(
        functools.partial(on_device, mesh.shape["patch"], mesh.shape["var"]),
        mesh=mesh, in_specs=in_specs, out_specs=out_specs, check_vma=False,
    )
```

```python
import functools

import jax
import jax.numpy as jnp
from jax import lax
from jax.experimental import pallas as pl
from jax.experimental.pallas import tpu as pltpu
from jax.sharding import PartitionSpec as P

HD = 64
REACH = 5
EPS = 1e-06
MESH = pl.DeviceIdType.MESH
F32 = jnp.float32
BF16 = jnp.bfloat16


def norm_rows(rows, gain):
    floats = rows.astype(F32)
    scaled = floats * lax.rsqrt(jnp.mean(floats * floats, axis=-1, keepdims=True) + EPS)
    return (scaled * gain).astype(BF16)


def dot(a, b):
    return jnp.dot(a, b, preferred_element_type=F32)


def dot_t(a, b):
    return lax.dot_general(a, b, (((1,), (1,)), ((), ())), preferred_element_type=F32)


def kernel(
    n, nvar, tok, marks, gids, tgain, sgain, wt, wot_in, wqs_in, wos_in,
    out, gx, mk, wot, wqs, wos, att, ratt, mid, sw, kvb, qb, prod, sc, pb,
    local_sem, tok_s, tok_r, mk_s, mk_r, w_s, w_r, att_s, att_r, win_s, win_r,
):
    me = lax.axis_index("patch")
    var = lax.axis_index("var")
    nv, pp, dm = tok.shape
    hw = wot_in.shape[0]
    heads = hw // HD
    side = (me + 1 - 2 * (me % 2), me + 2 - 4 * ((me // 2) % 2), n - 1 - me)
    sib = var + 1 - 2 * (var % 2)
    core = var % 2
    nbrs = (1, -1, 2, -2)

    def exists(k):
        return (var + k >= 0) & (var + k < nvar)

    barrier = pltpu.get_barrier_semaphore()
    count = n - 1 + 1
    for other in side:
        pl.semaphore_signal(barrier, inc=1, device_id={"patch": other}, device_id_type=MESH)
    pl.semaphore_signal(barrier, inc=1, device_id={"var": sib}, device_id_type=MESH)
    for k in nbrs:
        @pl.when(exists(k))
        def _():
            pl.semaphore_signal(barrier, inc=1, device_id={"var": var + k}, device_id_type=MESH)
        count = count + exists(k).astype(jnp.int32)
    own = [
        pltpu.make_async_copy(wot_in, wot.at[me], local_sem.at[0]),
        pltpu.make_async_copy(wqs_in, wqs.at[me], local_sem.at[1]),
        pltpu.make_async_copy(wos_in, wos.at[me], local_sem.at[2]),
    ]
    for c in own:
        c.start()
    pl.semaphore_wait(barrier, count)

    sends = []

    def remote(src, dst, ssem, rsem, **where):
        c = pltpu.make_async_remote_copy(
            src_ref=src, dst_ref=dst, send_sem=ssem, recv_sem=rsem, device_id=where, device_id_type=MESH
        )
        return c

    def launch(*a, **k):
        c = remote(*a, **k)
        c.start()
        sends.append(c)
        return c

    def block(of, lo=0, num=pp):
        return pl.ds(pl.multiple_of(of * pp + lo, num), num)

    half = pp // 2
    mk_c = [launch(marks, mk.at[me], mk_s.at[d], mk_r.at[d], patch=side[d]) for d in range(3)]
    tok_c = {}
    for i in range(nv):
        for d in (0, 1):
            v = i if d == 1 else nv - 1 - i
            tok_c[d, v] = launch(tok.at[v], gx.at[v, block(me), :], tok_s.at[d, v], tok_r.at[d, v], patch=side[d])
    routes = ((1, 0, 0, pp), (0, 2, 0, pp), (1, 1, 0, half), (0, 1, half, half))
    diag_c = []
    for i, (d, v, lo, num) in enumerate(routes):
        tok_c[d, v].wait_recv()
        piece = gx.at[v, block(side[d], lo, num), :]
        diag_c.append(launch(piece, piece, tok_s.at[2, i], tok_r.at[2, i], patch=side[1 - d]))

    arrays = ((wot_in, wot), (wqs_in, wqs), (wos_in, wos))
    wc = {}

    def piece_of(a, shard, part=None):
        rows = arrays[a][1].shape[1] // 2
        if part is None:
            return arrays[a][1].at[shard, pl.ds(pl.multiple_of(core * rows, rows), rows), :]
        num = rows // 2
        return arrays[a][1].at[shard, pl.ds(pl.multiple_of(core * rows + part * num, num), num), :]

    def w_own(a):
        src = arrays[a][0]
        rows = src.shape[0] // 2
        for d in (0, 1):
            wc[a, d] = launch(
                src.at[pl.ds(pl.multiple_of(core * rows, rows), rows), :], piece_of(a, me),
                w_s.at[a, d], w_r.at[a, d], patch=side[d],
            )

    def w_relay(a):
        for d in (0, 1):
            wc[a, d].wait_recv()
            piece = piece_of(a, side[d], 1 - d)
            wc[a, 2 + d] = launch(piece, piece, w_s.at[a, 2 + d], w_r.at[a, 2 + d], patch=side[1 - d])
            piece = piece_of(a, side[d])
            wc[a, 4 + d] = launch(piece, piece, w_s.at[a, 4 + d], w_r.at[a, 4 + d], var=sib)

    def w_diag(a):
        wc[a, 2].wait_recv()
        wc[a, 3].wait_recv()
        piece = piece_of(a, side[2])
        wc[a, 6] = launch(piece, piece, w_s.at[a, 6], w_r.at[a, 6], var=sib)

    w_own(0)
    for k in nbrs:
        lo = {1: 9, -1: 3, 2: 12, -2: 1}[k]
        num = nv if abs(k) == 1 else nv - 1

        @pl.when(jnp.logical_not(exists(k)))
        def _():
            sw[lo:lo + num] = jnp.zeros((num, pp, dm), BF16)

    gx[:, block(me), :] = tok[...]
    mk[me] = marks[...]
    for c in mk_c:
        c.wait_recv()
    for d in (0, 1):
        for v in range(nv):
            if (d, v) not in [r[:2] for r in routes]:
                tok_c[d, v].wait_recv()
    for c in diag_c:
        c.wait_recv()

    full = n * pp
    seen = jnp.concatenate([mk[s] for s in range(n)], axis=1)
    qi = lax.broadcasted_iota(jnp.int32, (full, full), 0)
    ki = lax.broadcasted_iota(jnp.int32, (full, full), 1)
    att_c = []
    for v in range(nv):
        normed = norm_rows(gx[v], tgain[...])
        proj = dot_t(normed, wt[...]).astype(BF16)
        allowed = ((ki < qi) & (seen[v:v + 1, :] > 0)) | (ki == qi)
        outs = []
        for h in range(heads):
            q = proj[:, h * HD:(h + 1) * HD]
            k = proj[:, hw + h * HD:hw + (h + 1) * HD]
            val = proj[:, 2 * hw + h * HD:2 * hw + (h + 1) * HD]
            s = lax.dot_general(q, k, (((1,), (1,)), ((), ())), preferred_element_type=F32) * HD ** (-0.5)
            s = jnp.where(allowed, s, -jnp.inf)
            e = jnp.exp(s - jnp.max(s, axis=-1, keepdims=True))
            w = (e / jnp.sum(e, axis=-1, keepdims=True)).astype(BF16)
            outs.append(dot(w, val).astype(BF16))
        att[v] = jnp.concatenate(outs, axis=1)
        for d in (2, 0, 1):
            att_c.append(launch(att.at[v, block(side[d]), :], ratt.at[me, v], att_s.at[v, d], att_r.at[v, d], patch=side[d]))
        ratt[me, v] = att[v, block(me), :]
    w_relay(0)
    w_own(1)
    own[0].wait()
    for c in att_c:
        c.wait_recv()
    w_diag(0)
    for k in (4, 5, 6):
        wc[0, k].wait_recv()

    rows = nv * pp
    mix = jnp.zeros((rows, dm), F32)
    for s in range(n):
        mix = mix + dot(ratt[s].reshape(rows, hw), wot[s]).astype(BF16).astype(F32)
    middle = (tok[...].reshape(rows, dm).astype(F32) + mix).astype(BF16)
    mid[...] = middle
    sw[6:6 + nv] = norm_rows(middle, sgain[...]).reshape(nv, pp, dm)

    def window(k, i):
        src = {1: (6, 9), -1: (6, 9), 2: (7, 9), -2: (6, 8)}[k]
        dst = {1: (3, 6), -1: (9, 12), 2: (1, 3), -2: (12, 14)}[k]
        return remote(sw.at[src[0]:src[1]], sw.at[dst[0]:dst[1]], win_s.at[i], win_r.at[i], var=var + k)

    for i, k in enumerate(nbrs):
        @pl.when(exists(k))
        def _():
            window(k, i).start()

    own[1].wait()
    own[2].wait()
    for i, k in enumerate(nbrs):
        @pl.when(exists(-k))
        def _():
            window(k, i).wait_recv()

    nkey = 4 + 3 * nv
    pairs = [(u, u + 6 + t) for u in range(nv) for t in range(-REACH, REACH + 1)]
    sc[...] = jnp.zeros_like(sc)

    def scores_of(s):
        qb[...] = dot_t(sw[6:6 + nv].reshape(rows, dm), wqs[s, :hw, :]).astype(BF16).reshape(nv, pp, hw)
        kvb[s] = dot_t(sw[1:1 + nkey].reshape(nkey * pp, dm), wqs[s, hw:, :]).astype(BF16).reshape(nkey, pp, 2 * hw)
        for i, (u, j) in enumerate(pairs):
            prod[i * pp:(i + 1) * pp, :] = (
                qb[u].astype(F32) * kvb[s, j - 1, :, :hw].astype(F32)
            ).astype(BF16)
        lane = lax.broadcasted_iota(jnp.int32, (hw, 128), 0) // HD + heads * s
        col = lax.broadcasted_iota(jnp.int32, (hw, 128), 1)
        sc[...] += dot(prod[...], (lane == col).astype(F32).astype(BF16))

    scores_of(me)
    w_relay(1)
    w_own(2)
    for d in (0, 1):
        wc[1, 4 + d].wait_recv()
        scores_of(side[d])
    w_diag(1)
    wc[1, 6].wait_recv()
    scores_of(side[2])
    w_relay(2)

    total = gids.shape[0]
    local_n = total // nv
    base = (var % local_n) * nv
    for u in range(nv):
        mine_group = gids[base + u]
        slabs = []
        for t in range(-REACH, REACH + 1):
            w = base + u + t
            inside = (w >= 0) & (w < total)
            at = jnp.minimum(jnp.maximum(w, 0), total - 1)
            i = pairs.index((u, u + 6 + t))
            ok = inside & (gids[at] == mine_group)
            slabs.append(jnp.where(ok, sc[i * pp:(i + 1) * pp, :] * HD ** (-0.5), -jnp.inf))
        top = functools.reduce(jnp.maximum, slabs)
        es = [jnp.exp(x - top) for x in slabs]
        den = functools.reduce(lambda a, b: a + b, es)
        for t, e in enumerate(es):
            i = u * (2 * REACH + 1) + t
            pb[i * pp:(i + 1) * pp, :] = (e / den).astype(BF16)

    def mix_of(s):
        lane = lax.broadcasted_iota(jnp.int32, (128, hw), 1) // HD + heads * s
        col = lax.broadcasted_iota(jnp.int32, (128, hw), 0)
        spread = (lane == col).astype(F32).astype(BF16)
        done = []
        for u in range(nv):
            total_u = jnp.zeros((pp, hw), F32)
            lo = u * (2 * REACH + 1)
            wide = dot(pb[lo * pp:(lo + 2 * REACH + 1) * pp, :], spread)
            for t in range(2 * REACH + 1):
                val = kvb[s, u + t, :, hw:].astype(F32)
                total_u = total_u + wide[t * pp:(t + 1) * pp] * val
            done.append(total_u.astype(BF16))
        res = dot(jnp.concatenate(done, axis=0), wos[s]).astype(BF16).astype(F32)
        return res

    mix2 = mix_of(me)
    for d in (0, 1):
        wc[2, 4 + d].wait_recv()
        mix2 = mix2 + mix_of(side[d])
    w_diag(2)
    wc[2, 6].wait_recv()
    mix2 = mix2 + mix_of(side[2])
    out[...] = (mid[...].astype(F32) + mix2).astype(BF16).reshape(nv, pp, dm)

    for c in sends:
        c.wait_send()
    for i, k in enumerate(nbrs):
        @pl.when(exists(k))
        def _():
            window(k, i).wait_send()


def on_device(n, nvar, tokens, patch_mask, group_ids, time_gain, time_qkv, time_out, space_gain, space_qkv, space_out):
    pp, nv, dm = tokens.shape
    hw = time_out.shape[0]
    tok = jnp.transpose(tokens, (1, 0, 2))
    wt = jnp.transpose(time_qkv, (1, 2, 0)).reshape(3 * hw, dm)
    wqs = jnp.transpose(space_qkv, (1, 2, 0)).reshape(3 * hw, dm)
    npair = nv * (2 * REACH + 1)
    vm = pl.BlockSpec(memory_space=pltpu.VMEM)
    anyv = pl.BlockSpec(memory_space=pl.ANY)
    dma = pltpu.SemaphoreType.DMA
    res = pl.pallas_call(
        functools.partial(kernel, n, nvar),
        out_shape=jax.ShapeDtypeStruct((nv, pp, dm), BF16),
        in_specs=[vm, vm, pl.BlockSpec(memory_space=pltpu.SMEM), vm, vm, vm, anyv, anyv, anyv],
        out_specs=vm,
        scratch_shapes=[
            pltpu.VMEM((nv, n * pp, dm), BF16),
            pltpu.VMEM((n, nv, pp), jnp.int32),
            pltpu.VMEM((n, hw, dm), BF16),
            pltpu.VMEM((n, 3 * hw, dm), BF16),
            pltpu.VMEM((n, hw, dm), BF16),
            pltpu.VMEM((nv, n * pp, hw), BF16),
            pltpu.VMEM((n, nv, pp, hw), BF16),
            pltpu.VMEM((nv * pp, dm), BF16),
            pltpu.VMEM((5 * nv, pp, dm), BF16),
            pltpu.VMEM((n, 4 + 3 * nv, pp, 2 * hw), BF16),
            pltpu.VMEM((nv, pp, hw), BF16),
            pltpu.VMEM((npair * pp, hw), BF16),
            pltpu.VMEM((npair * pp, 128), F32),
            pltpu.VMEM((npair * pp, 128), BF16),
            dma((3,)), dma((3, 4)), dma((3, 4)), dma((3,)), dma((3,)),
            dma((3, 7)), dma((3, 7)), dma((nv, 3)), dma((nv, 3)), dma((4,)), dma((4,)),
        ],
        compiler_params=pltpu.CompilerParams(
            collective_id=0, has_side_effects=True, vmem_limit_bytes=52 * 2**20
        ),
    )(tok, patch_mask.T, group_ids, time_gain, space_gain, wt, time_out, wqs, space_out)
    return jnp.transpose(res, (1, 0, 2))


def solution(mesh):
    in_specs = (
        P("patch", ("parts", "var"), None),
        P("patch", ("parts", "var")),
        P("parts"),
        P(),
        P(None, None, "patch"),
        P("patch", None),
        P(),
        P(None, None, "patch"),
        P("patch", None),
    )
    out_specs = P("patch", ("parts", "var"), None)
    return jax.shard_map(
        functools.partial(on_device, mesh.shape["patch"], mesh.shape["var"]),
        mesh=mesh, in_specs=in_specs, out_specs=out_specs, check_vma=False,
    )
```

```python
import functools

import jax
import jax.numpy as jnp
from jax import lax
from jax.experimental import pallas as pl
from jax.experimental.pallas import tpu as pltpu
from jax.sharding import PartitionSpec as P

HD = 64
REACH = 5
EPS = 1e-06
MESH = pl.DeviceIdType.MESH
F32 = jnp.float32
BF16 = jnp.bfloat16


def norm_rows(rows, gain):
    floats = rows.astype(F32)
    scaled = floats * lax.rsqrt(jnp.mean(floats * floats, axis=-1, keepdims=True) + EPS)
    return (scaled * gain).astype(BF16)


def dot(a, b):
    return jnp.dot(a, b, preferred_element_type=F32)


def dot_t(a, b):
    return lax.dot_general(a, b, (((1,), (1,)), ((), ())), preferred_element_type=F32)


def kernel(
    n, nvar, tok, marks, gids, tgain, sgain, wt_in, wot_in, wqs_in, wos_in,
    out, gx, mk, wt, wot, wqs, wos, att, ratt, mid, sw, kvb, qb, prod, sc, pb,
    local_sem, tok_s, tok_r, mk_s, mk_r, w_s, w_r, att_s, att_r, win_s, win_r,
):
    me = lax.axis_index("patch")
    var = lax.axis_index("var")
    nv, pp, dm = tok.shape
    hw = wot_in.shape[0]
    heads = hw // HD
    side = (me + 1 - 2 * (me % 2), me + 2 - 4 * ((me // 2) % 2), n - 1 - me)
    sib = var + 1 - 2 * (var % 2)
    core = var % 2
    nbrs = (1, -1, 2, -2)

    def exists(k):
        return (var + k >= 0) & (var + k < nvar)

    barrier = pltpu.get_barrier_semaphore()
    count = n - 1 + 1
    for other in side:
        pl.semaphore_signal(barrier, inc=1, device_id={"patch": other}, device_id_type=MESH)
    pl.semaphore_signal(barrier, inc=1, device_id={"var": sib}, device_id_type=MESH)
    for k in nbrs:
        @pl.when(exists(k))
        def _():
            pl.semaphore_signal(barrier, inc=1, device_id={"var": var + k}, device_id_type=MESH)
        count = count + exists(k).astype(jnp.int32)
    own = [
        pltpu.make_async_copy(wot_in, wot.at[me], local_sem.at[0]),
        pltpu.make_async_copy(wqs_in, wqs.at[me], local_sem.at[1]),
        pltpu.make_async_copy(wos_in, wos.at[me], local_sem.at[2]),
        pltpu.make_async_copy(wt_in, wt, local_sem.at[3]),
        pltpu.make_async_copy(tok, gx.at[:, pl.ds(pl.multiple_of(me * pp, pp), pp), :], local_sem.at[4]),
    ]
    for i in (4, 3, 0, 1, 2):
        own[i].start()
    pl.semaphore_wait(barrier, count)

    sends = []

    def remote(src, dst, ssem, rsem, **where):
        c = pltpu.make_async_remote_copy(
            src_ref=src, dst_ref=dst, send_sem=ssem, recv_sem=rsem, device_id=where, device_id_type=MESH
        )
        return c

    def launch(*a, **k):
        c = remote(*a, **k)
        c.start()
        sends.append(c)
        return c

    def block(of, lo=0, num=pp):
        return pl.ds(pl.multiple_of(of * pp + lo, num), num)

    half = pp // 2
    mk_c = [launch(marks, mk.at[me], mk_s.at[d], mk_r.at[d], patch=side[d]) for d in range(3)]
    tok_c = {}
    for i in range(nv):
        for d in (0, 1):
            v = i if d == 1 else nv - 1 - i
            tok_c[d, v] = launch(tok.at[v], gx.at[v, block(me), :], tok_s.at[d, v], tok_r.at[d, v], patch=side[d])
    routes = ((1, 0, 0, pp), (0, 2, 0, pp), (1, 1, 0, half), (0, 1, half, half))
    diag_c = []
    for i, (d, v, lo, num) in enumerate(routes):
        tok_c[d, v].wait_recv()
        piece = gx.at[v, block(side[d], lo, num), :]
        diag_c.append(launch(piece, piece, tok_s.at[2, i], tok_r.at[2, i], patch=side[1 - d]))

    arrays = ((wot_in, wot), (wqs_in, wqs), (wos_in, wos))
    wc = {}

    def piece_of(a, shard, part=None):
        rows = arrays[a][1].shape[1] // 2
        if part is None:
            return arrays[a][1].at[shard, pl.ds(pl.multiple_of(core * rows, rows), rows), :]
        num = rows // 2
        return arrays[a][1].at[shard, pl.ds(pl.multiple_of(core * rows + part * num, num), num), :]

    def w_own(a):
        src = arrays[a][0]
        rows = src.shape[0] // 2
        for d in (0, 1):
            wc[a, d] = launch(
                src.at[pl.ds(pl.multiple_of(core * rows, rows), rows), :], piece_of(a, me),
                w_s.at[a, d], w_r.at[a, d], patch=side[d],
            )

    def w_relay(a):
        for d in (0, 1):
            wc[a, d].wait_recv()
            piece = piece_of(a, side[d], 1 - d)
            wc[a, 2 + d] = launch(piece, piece, w_s.at[a, 2 + d], w_r.at[a, 2 + d], patch=side[1 - d])
            piece = piece_of(a, side[d])
            wc[a, 4 + d] = launch(piece, piece, w_s.at[a, 4 + d], w_r.at[a, 4 + d], var=sib)

    def w_diag(a):
        wc[a, 2].wait_recv()
        wc[a, 3].wait_recv()
        piece = piece_of(a, side[2])
        wc[a, 6] = launch(piece, piece, w_s.at[a, 6], w_r.at[a, 6], var=sib)

    w_own(0)
    for k in nbrs:
        lo = {1: 9, -1: 3, 2: 12, -2: 1}[k]
        num = nv if abs(k) == 1 else nv - 1

        @pl.when(jnp.logical_not(exists(k)))
        def _():
            sw[lo:lo + num] = jnp.zeros((num, pp, dm), BF16)

    mk[me] = marks[...]
    own[3].wait()
    own[4].wait()
    for c in mk_c:
        c.wait_recv()
    for d in (0, 1):
        for v in range(nv):
            if (d, v) not in [r[:2] for r in routes]:
                tok_c[d, v].wait_recv()
    for c in diag_c:
        c.wait_recv()

    full = n * pp
    seen = jnp.concatenate([mk[s] for s in range(n)], axis=1)
    qi = lax.broadcasted_iota(jnp.int32, (full, full), 0)
    ki = lax.broadcasted_iota(jnp.int32, (full, full), 1)
    att_c = []
    for v in range(nv):
        normed = norm_rows(gx[v], tgain[...])
        proj = dot_t(normed, wt[...]).astype(BF16)
        allowed = ((ki < qi) & (seen[v:v + 1, :] > 0)) | (ki == qi)
        outs = []
        for h in range(heads):
            q = proj[:, h * HD:(h + 1) * HD]
            k = proj[:, hw + h * HD:hw + (h + 1) * HD]
            val = proj[:, 2 * hw + h * HD:2 * hw + (h + 1) * HD]
            s = lax.dot_general(q, k, (((1,), (1,)), ((), ())), preferred_element_type=F32) * HD ** (-0.5)
            s = jnp.where(allowed, s, -jnp.inf)
            e = jnp.exp(s - jnp.max(s, axis=-1, keepdims=True))
            w = (e / jnp.sum(e, axis=-1, keepdims=True)).astype(BF16)
            outs.append(dot(w, val).astype(BF16))
        att[v] = jnp.concatenate(outs, axis=1)
        for d in (2, 0, 1):
            att_c.append(launch(att.at[v, block(side[d]), :], ratt.at[me, v], att_s.at[v, d], att_r.at[v, d], patch=side[d]))
        ratt[me, v] = att[v, block(me), :]
    w_relay(0)
    w_own(1)
    own[0].wait()
    for c in att_c:
        c.wait_recv()
    w_diag(0)
    for k in (4, 5, 6):
        wc[0, k].wait_recv()

    rows = nv * pp
    mix = jnp.zeros((rows, dm), F32)
    for s in range(n):
        mix = mix + dot(ratt[s].reshape(rows, hw), wot[s]).astype(BF16).astype(F32)
    middle = (gx[:, block(me), :].reshape(rows, dm).astype(F32) + mix).astype(BF16)
    mid[...] = middle
    sw[6:6 + nv] = norm_rows(middle, sgain[...]).reshape(nv, pp, dm)

    def window(k, i):
        src = {1: (6, 9), -1: (6, 9), 2: (7, 9), -2: (6, 8)}[k]
        dst = {1: (3, 6), -1: (9, 12), 2: (1, 3), -2: (12, 14)}[k]
        return remote(sw.at[src[0]:src[1]], sw.at[dst[0]:dst[1]], win_s.at[i], win_r.at[i], var=var + k)

    for i, k in enumerate(nbrs):
        @pl.when(exists(k))
        def _():
            window(k, i).start()

    w_own(2)
    own[1].wait()
    own[2].wait()
    w_relay(1)
    for i, k in enumerate(nbrs):
        @pl.when(exists(-k))
        def _():
            window(k, i).wait_recv()

    nkey = 4 + 3 * nv
    pairs = [(u, u + 6 + t) for u in range(nv) for t in range(-REACH, REACH + 1)]
    sc[...] = jnp.zeros_like(sc)

    def scores_of(s):
        qb[...] = dot_t(sw[6:6 + nv].reshape(rows, dm), wqs[s, :hw, :]).astype(BF16).reshape(nv, pp, hw)
        kvb[s] = dot_t(sw[1:1 + nkey].reshape(nkey * pp, dm), wqs[s, hw:, :]).astype(BF16).reshape(nkey, pp, 2 * hw)
        for i, (u, j) in enumerate(pairs):
            prod[i * pp:(i + 1) * pp, :] = (
                qb[u].astype(F32) * kvb[s, j - 1, :, :hw].astype(F32)
            ).astype(BF16)
        lane = lax.broadcasted_iota(jnp.int32, (hw, 128), 0) // HD + heads * s
        col = lax.broadcasted_iota(jnp.int32, (hw, 128), 1)
        sc[...] += dot(prod[...], (lane == col).astype(F32).astype(BF16))

    def soften():
        total = gids.shape[0]
        local_n = total // nv
        base = (var % local_n) * nv
        for u in range(nv):
            mine_group = gids[base + u]
            slabs = []
            for t in range(-REACH, REACH + 1):
                w = base + u + t
                inside = (w >= 0) & (w < total)
                at = jnp.minimum(jnp.maximum(w, 0), total - 1)
                i = pairs.index((u, u + 6 + t))
                ok = inside & (gids[at] == mine_group)
                slabs.append(jnp.where(ok, sc[i * pp:(i + 1) * pp, :] * HD ** (-0.5), -jnp.inf))
            top = functools.reduce(jnp.maximum, slabs)
            es = [jnp.exp(x - top) for x in slabs]
            den = functools.reduce(lambda a, b: a + b, es)
            for t, e in enumerate(es):
                i = u * (2 * REACH + 1) + t
                pb[i * pp:(i + 1) * pp, :] = (e / den).astype(BF16)

    def mix_of(s):
        lane = lax.broadcasted_iota(jnp.int32, (128, hw), 1) // HD + heads * s
        col = lax.broadcasted_iota(jnp.int32, (128, hw), 0)
        spread = (lane == col).astype(F32).astype(BF16)
        done = []
        for u in range(nv):
            total_u = jnp.zeros((pp, hw), F32)
            lo = u * (2 * REACH + 1)
            wide = dot(pb[lo * pp:(lo + 2 * REACH + 1) * pp, :], spread)
            for t in range(2 * REACH + 1):
                val = kvb[s, u + t, :, hw:].astype(F32)
                total_u = total_u + wide[t * pp:(t + 1) * pp] * val
            done.append(total_u.astype(BF16))
        res = dot(jnp.concatenate(done, axis=0), wos[s]).astype(BF16).astype(F32)
        return res

    scores_of(me)
    for d in (0, 1):
        wc[1, 4 + d].wait_recv()
        scores_of(side[d])
    soften()
    mix2 = mix_of(me)
    w_relay(2)
    for d in (0, 1):
        wc[2, 4 + d].wait_recv()
        mix2 = mix2 + mix_of(side[d])
    w_diag(1)
    w_diag(2)
    wc[1, 6].wait_recv()
    scores_of(side[2])
    soften()
    wc[2, 6].wait_recv()
    mix2 = mix2 + mix_of(side[2])
    out[...] = (mid[...].astype(F32) + mix2).astype(BF16).reshape(nv, pp, dm)

    for c in sends:
        c.wait_send()
    for i, k in enumerate(nbrs):
        @pl.when(exists(k))
        def _():
            window(k, i).wait_send()


def on_device(n, nvar, tokens, patch_mask, group_ids, time_gain, time_qkv, time_out, space_gain, space_qkv, space_out):
    pp, nv, dm = tokens.shape
    hw = time_out.shape[0]
    tok = jnp.transpose(tokens, (1, 0, 2))
    wt = jnp.transpose(time_qkv, (1, 2, 0)).reshape(3 * hw, dm)
    wqs = jnp.transpose(space_qkv, (1, 2, 0)).reshape(3 * hw, dm)
    npair = nv * (2 * REACH + 1)
    vm = pl.BlockSpec(memory_space=pltpu.VMEM)
    anyv = pl.BlockSpec(memory_space=pltpu.HBM)
    dma = pltpu.SemaphoreType.DMA
    res = pl.pallas_call(
        functools.partial(kernel, n, nvar),
        out_shape=jax.ShapeDtypeStruct((nv, pp, dm), BF16),
        in_specs=[anyv, vm, pl.BlockSpec(memory_space=pltpu.SMEM), vm, vm, anyv, anyv, anyv, anyv],
        out_specs=vm,
        scratch_shapes=[
            pltpu.VMEM((nv, n * pp, dm), BF16),
            pltpu.VMEM((n, nv, pp), jnp.int32),
            pltpu.VMEM((3 * hw, dm), BF16),
            pltpu.VMEM((n, hw, dm), BF16),
            pltpu.VMEM((n, 3 * hw, dm), BF16),
            pltpu.VMEM((n, hw, dm), BF16),
            pltpu.VMEM((nv, n * pp, hw), BF16),
            pltpu.VMEM((n, nv, pp, hw), BF16),
            pltpu.VMEM((nv * pp, dm), BF16),
            pltpu.VMEM((5 * nv, pp, dm), BF16),
            pltpu.VMEM((n, 4 + 3 * nv, pp, 2 * hw), BF16),
            pltpu.VMEM((nv, pp, hw), BF16),
            pltpu.VMEM((npair * pp, hw), BF16),
            pltpu.VMEM((npair * pp, 128), F32),
            pltpu.VMEM((npair * pp, 128), BF16),
            dma((5,)), dma((3, 4)), dma((3, 4)), dma((3,)), dma((3,)),
            dma((3, 7)), dma((3, 7)), dma((nv, 3)), dma((nv, 3)), dma((4,)), dma((4,)),
        ],
        compiler_params=pltpu.CompilerParams(
            collective_id=0, has_side_effects=True, vmem_limit_bytes=67_000_000
        ),
    )(tok, patch_mask.T, group_ids, time_gain, space_gain, wt, time_out, wqs, space_out)
    return jnp.transpose(res, (1, 0, 2))


def solution(mesh):
    in_specs = (
        P("patch", ("parts", "var"), None),
        P("patch", ("parts", "var")),
        P("parts"),
        P(),
        P(None, None, "patch"),
        P("patch", None),
        P(),
        P(None, None, "patch"),
        P("patch", None),
    )
    out_specs = P("patch", ("parts", "var"), None)
    return jax.shard_map(
        functools.partial(on_device, mesh.shape["patch"], mesh.shape["var"]),
        mesh=mesh, in_specs=in_specs, out_specs=out_specs, check_vma=False,
    )
```

```python
import functools

import jax
import jax.numpy as jnp
from jax import lax
from jax.experimental import pallas as pl
from jax.experimental.pallas import tpu as pltpu
from jax.sharding import PartitionSpec as P

HD = 64
REACH = 5
EPS = 1e-06
MESH = pl.DeviceIdType.MESH
F32 = jnp.float32
BF16 = jnp.bfloat16


def norm_rows(rows, gain):
    floats = rows.astype(F32)
    scaled = floats * lax.rsqrt(jnp.mean(floats * floats, axis=-1, keepdims=True) + EPS)
    return (scaled * gain).astype(BF16)


def dot(a, b):
    return jnp.dot(a, b, preferred_element_type=F32)


def dot_t(a, b):
    return lax.dot_general(a, b, (((1,), (1,)), ((), ())), preferred_element_type=F32)


def kernel(
    n, nvar, tok, marks, gids, tgain, sgain, wt_in, wot_in, wqs_in, wos_in,
    out, gx, mk, wt, wot, wqs, wos, att, ratt, mid, sw, kvb, qb, prod, sc, pb,
    local_sem, tok_s, tok_r, mk_s, mk_r, w_s, w_r, att_s, att_r, win_s, win_r,
):
    me = lax.axis_index("patch")
    var = lax.axis_index("var")
    nv, pp, dm = tok.shape
    hw = wot_in.shape[0]
    heads = hw // HD
    side = (me + 1 - 2 * (me % 2), me + 2 - 4 * ((me // 2) % 2), n - 1 - me)
    sib = var + 1 - 2 * (var % 2)
    core = var % 2
    nbrs = (1, -1, 2, -2)

    def exists(k):
        return (var + k >= 0) & (var + k < nvar)

    barrier = pltpu.get_barrier_semaphore()
    count = n - 1 + 1
    for other in side:
        pl.semaphore_signal(barrier, inc=1, device_id={"patch": other}, device_id_type=MESH)
    pl.semaphore_signal(barrier, inc=1, device_id={"var": sib}, device_id_type=MESH)
    for k in nbrs:
        @pl.when(exists(k))
        def _():
            pl.semaphore_signal(barrier, inc=1, device_id={"var": var + k}, device_id_type=MESH)
        count = count + exists(k).astype(jnp.int32)
    own = [
        pltpu.make_async_copy(wot_in, wot.at[me], local_sem.at[0]),
        pltpu.make_async_copy(wqs_in, wqs.at[me], local_sem.at[1]),
        pltpu.make_async_copy(wos_in, wos.at[me], local_sem.at[2]),
        pltpu.make_async_copy(wt_in, wt, local_sem.at[3]),
        pltpu.make_async_copy(tok, gx.at[:, pl.ds(pl.multiple_of(me * pp, pp), pp), :], local_sem.at[4]),
    ]
    for i in (4, 3, 0, 1, 2):
        own[i].start()
    pl.semaphore_wait(barrier, count)

    sends = []

    def remote(src, dst, ssem, rsem, **where):
        c = pltpu.make_async_remote_copy(
            src_ref=src, dst_ref=dst, send_sem=ssem, recv_sem=rsem, device_id=where, device_id_type=MESH
        )
        return c

    def launch(*a, **k):
        c = remote(*a, **k)
        c.start()
        sends.append(c)
        return c

    def block(of, lo=0, num=pp):
        return pl.ds(pl.multiple_of(of * pp + lo, num), num)

    half = pp // 2
    mk_c = [launch(marks, mk.at[me], mk_s.at[d], mk_r.at[d], patch=side[d]) for d in range(3)]
    tok_c = {}
    for i in range(nv):
        for d in (0, 1):
            v = i if d == 1 else nv - 1 - i
            tok_c[d, v] = launch(tok.at[v], gx.at[v, block(me), :], tok_s.at[d, v], tok_r.at[d, v], patch=side[d])
    routes = ((1, 0, 0, pp), (0, 2, 0, pp), (1, 1, 0, half), (0, 1, half, half))
    diag_c = []
    for i, (d, v, lo, num) in enumerate(routes):
        tok_c[d, v].wait_recv()
        piece = gx.at[v, block(side[d], lo, num), :]
        diag_c.append(launch(piece, piece, tok_s.at[2, i], tok_r.at[2, i], patch=side[1 - d]))

    arrays = ((wot_in, wot), (wqs_in, wqs), (wos_in, wos))
    wc = {}

    def piece_of(a, shard, part=None):
        rows = arrays[a][1].shape[1] // 2
        if part is None:
            return arrays[a][1].at[shard, pl.ds(pl.multiple_of(core * rows, rows), rows), :]
        num = rows // 2
        return arrays[a][1].at[shard, pl.ds(pl.multiple_of(core * rows + part * num, num), num), :]

    def w_own(a):
        src = arrays[a][0]
        rows = src.shape[0] // 2
        for d in (0, 1):
            wc[a, d] = launch(
                src.at[pl.ds(pl.multiple_of(core * rows, rows), rows), :], piece_of(a, me),
                w_s.at[a, d], w_r.at[a, d], patch=side[d],
            )

    def w_relay(a):
        for d in (0, 1):
            wc[a, d].wait_recv()
            piece = piece_of(a, side[d], 1 - d)
            wc[a, 2 + d] = launch(piece, piece, w_s.at[a, 2 + d], w_r.at[a, 2 + d], patch=side[1 - d])
            piece = piece_of(a, side[d])
            wc[a, 4 + d] = launch(piece, piece, w_s.at[a, 4 + d], w_r.at[a, 4 + d], var=sib)

    def w_diag(a):
        wc[a, 2].wait_recv()
        wc[a, 3].wait_recv()
        piece = piece_of(a, side[2])
        wc[a, 6] = launch(piece, piece, w_s.at[a, 6], w_r.at[a, 6], var=sib)

    w_own(0)
    w_own(2)
    for k in nbrs:
        lo = {1: 9, -1: 3, 2: 12, -2: 1}[k]
        num = nv if abs(k) == 1 else nv - 1

        @pl.when(jnp.logical_not(exists(k)))
        def _():
            sw[lo:lo + num] = jnp.zeros((num, pp, dm), BF16)

    mk[me] = marks[...]
    own[3].wait()
    own[4].wait()
    for c in mk_c:
        c.wait_recv()
    for d in (0, 1):
        for v in range(nv):
            if (d, v) not in [r[:2] for r in routes]:
                tok_c[d, v].wait_recv()
    for c in diag_c:
        c.wait_recv()

    full = n * pp
    seen = jnp.concatenate([mk[s] for s in range(n)], axis=1)
    qi = lax.broadcasted_iota(jnp.int32, (full, full), 0)
    ki = lax.broadcasted_iota(jnp.int32, (full, full), 1)
    att_c = []
    for v in range(nv):
        normed = norm_rows(gx[v], tgain[...])
        proj = dot_t(normed, wt[...]).astype(BF16)
        allowed = ((ki < qi) & (seen[v:v + 1, :] > 0)) | (ki == qi)
        outs = []
        for h in range(heads):
            q = proj[:, h * HD:(h + 1) * HD]
            k = proj[:, hw + h * HD:hw + (h + 1) * HD]
            val = proj[:, 2 * hw + h * HD:2 * hw + (h + 1) * HD]
            s = lax.dot_general(q, k, (((1,), (1,)), ((), ())), preferred_element_type=F32) * HD ** (-0.5)
            s = jnp.where(allowed, s, -jnp.inf)
            e = jnp.exp(s - jnp.max(s, axis=-1, keepdims=True))
            w = (e / jnp.sum(e, axis=-1, keepdims=True)).astype(BF16)
            outs.append(dot(w, val).astype(BF16))
        att[v] = jnp.concatenate(outs, axis=1)
        for d in (2, 0, 1):
            att_c.append(launch(att.at[v, block(side[d]), :], ratt.at[me, v], att_s.at[v, d], att_r.at[v, d], patch=side[d]))
        ratt[me, v] = att[v, block(me), :]
    w_relay(0)
    w_own(1)
    own[0].wait()
    for c in att_c:
        c.wait_recv()
    w_diag(0)
    for k in (4, 5, 6):
        wc[0, k].wait_recv()

    rows = nv * pp
    mix = jnp.zeros((rows, dm), F32)
    for s in range(n):
        mix = mix + dot(ratt[s].reshape(rows, hw), wot[s]).astype(BF16).astype(F32)
    middle = (gx[:, block(me), :].reshape(rows, dm).astype(F32) + mix).astype(BF16)
    mid[...] = middle
    sw[6:6 + nv] = norm_rows(middle, sgain[...]).reshape(nv, pp, dm)

    def window(k, i):
        src = {1: (6, 9), -1: (6, 9), 2: (7, 9), -2: (6, 8)}[k]
        dst = {1: (3, 6), -1: (9, 12), 2: (1, 3), -2: (12, 14)}[k]
        return remote(sw.at[src[0]:src[1]], sw.at[dst[0]:dst[1]], win_s.at[i], win_r.at[i], var=var + k)

    for i, k in enumerate(nbrs):
        @pl.when(exists(k))
        def _():
            window(k, i).start()

    own[1].wait()
    own[2].wait()
    w_relay(1)
    w_relay(2)
    for i, k in enumerate(nbrs):
        @pl.when(exists(-k))
        def _():
            window(k, i).wait_recv()

    nkey = 4 + 3 * nv
    pairs = [(u, u + 6 + t) for u in range(nv) for t in range(-REACH, REACH + 1)]
    sc[...] = jnp.zeros_like(sc)

    def scores_of(s):
        qb[...] = dot_t(sw[6:6 + nv].reshape(rows, dm), wqs[s, :hw, :]).astype(BF16).reshape(nv, pp, hw)
        kvb[s] = dot_t(sw[1:1 + nkey].reshape(nkey * pp, dm), wqs[s, hw:, :]).astype(BF16).reshape(nkey, pp, 2 * hw)
        for i, (u, j) in enumerate(pairs):
            prod[i * pp:(i + 1) * pp, :] = (
                qb[u].astype(F32) * kvb[s, j - 1, :, :hw].astype(F32)
            ).astype(BF16)
        lane = lax.broadcasted_iota(jnp.int32, (hw, 128), 0) // HD + heads * s
        col = lax.broadcasted_iota(jnp.int32, (hw, 128), 1)
        sc[...] += dot(prod[...], (lane == col).astype(F32).astype(BF16))

    def soften():
        total = gids.shape[0]
        local_n = total // nv
        base = (var % local_n) * nv
        for u in range(nv):
            mine_group = gids[base + u]
            slabs = []
            for t in range(-REACH, REACH + 1):
                w = base + u + t
                inside = (w >= 0) & (w < total)
                at = jnp.minimum(jnp.maximum(w, 0), total - 1)
                i = pairs.index((u, u + 6 + t))
                ok = inside & (gids[at] == mine_group)
                slabs.append(jnp.where(ok, sc[i * pp:(i + 1) * pp, :] * HD ** (-0.5), -jnp.inf))
            top = functools.reduce(jnp.maximum, slabs)
            es = [jnp.exp(x - top) for x in slabs]
            den = functools.reduce(lambda a, b: a + b, es)
            for t, e in enumerate(es):
                i = u * (2 * REACH + 1) + t
                pb[i * pp:(i + 1) * pp, :] = (e / den).astype(BF16)

    def mix_of(s):
        lane = lax.broadcasted_iota(jnp.int32, (128, hw), 1) // HD + heads * s
        col = lax.broadcasted_iota(jnp.int32, (128, hw), 0)
        spread = (lane == col).astype(F32).astype(BF16)
        done = []
        for u in range(nv):
            total_u = jnp.zeros((pp, hw), F32)
            lo = u * (2 * REACH + 1)
            wide = dot(pb[lo * pp:(lo + 2 * REACH + 1) * pp, :], spread)
            for t in range(2 * REACH + 1):
                val = kvb[s, u + t, :, hw:].astype(F32)
                total_u = total_u + wide[t * pp:(t + 1) * pp] * val
            done.append(total_u.astype(BF16))
        res = dot(jnp.concatenate(done, axis=0), wos[s]).astype(BF16).astype(F32)
        return res

    scores_of(me)
    for d in (0, 1):
        wc[1, 4 + d].wait_recv()
        scores_of(side[d])
    soften()
    mix2 = mix_of(me)
    for d in (0, 1):
        wc[2, 4 + d].wait_recv()
        mix2 = mix2 + mix_of(side[d])
    w_diag(1)
    w_diag(2)
    wc[1, 6].wait_recv()
    scores_of(side[2])
    soften()
    wc[2, 6].wait_recv()
    mix2 = mix2 + mix_of(side[2])
    out[...] = (mid[...].astype(F32) + mix2).astype(BF16).reshape(nv, pp, dm)

    for c in sends:
        c.wait_send()
    for i, k in enumerate(nbrs):
        @pl.when(exists(k))
        def _():
            window(k, i).wait_send()


def on_device(n, nvar, tokens, patch_mask, group_ids, time_gain, time_qkv, time_out, space_gain, space_qkv, space_out):
    pp, nv, dm = tokens.shape
    hw = time_out.shape[0]
    tok = jnp.transpose(tokens, (1, 0, 2))
    wt = jnp.transpose(time_qkv, (1, 2, 0)).reshape(3 * hw, dm)
    wqs = jnp.transpose(space_qkv, (1, 2, 0)).reshape(3 * hw, dm)
    npair = nv * (2 * REACH + 1)
    vm = pl.BlockSpec(memory_space=pltpu.VMEM)
    anyv = pl.BlockSpec(memory_space=pltpu.HBM)
    dma = pltpu.SemaphoreType.DMA
    res = pl.pallas_call(
        functools.partial(kernel, n, nvar),
        out_shape=jax.ShapeDtypeStruct((nv, pp, dm), BF16),
        in_specs=[anyv, vm, pl.BlockSpec(memory_space=pltpu.SMEM), vm, vm, anyv, anyv, anyv, anyv],
        out_specs=vm,
        scratch_shapes=[
            pltpu.VMEM((nv, n * pp, dm), BF16),
            pltpu.VMEM((n, nv, pp), jnp.int32),
            pltpu.VMEM((3 * hw, dm), BF16),
            pltpu.VMEM((n, hw, dm), BF16),
            pltpu.VMEM((n, 3 * hw, dm), BF16),
            pltpu.VMEM((n, hw, dm), BF16),
            pltpu.VMEM((nv, n * pp, hw), BF16),
            pltpu.VMEM((n, nv, pp, hw), BF16),
            pltpu.VMEM((nv * pp, dm), BF16),
            pltpu.VMEM((5 * nv, pp, dm), BF16),
            pltpu.VMEM((n, 4 + 3 * nv, pp, 2 * hw), BF16),
            pltpu.VMEM((nv, pp, hw), BF16),
            pltpu.VMEM((npair * pp, hw), BF16),
            pltpu.VMEM((npair * pp, 128), F32),
            pltpu.VMEM((npair * pp, 128), BF16),
            dma((5,)), dma((3, 4)), dma((3, 4)), dma((3,)), dma((3,)),
            dma((3, 7)), dma((3, 7)), dma((nv, 3)), dma((nv, 3)), dma((4,)), dma((4,)),
        ],
        compiler_params=pltpu.CompilerParams(
            collective_id=0, has_side_effects=True, vmem_limit_bytes=67_000_000
        ),
    )(tok, patch_mask.T, group_ids, time_gain, space_gain, wt, time_out, wqs, space_out)
    return jnp.transpose(res, (1, 0, 2))


def solution(mesh):
    in_specs = (
        P("patch", ("parts", "var"), None),
        P("patch", ("parts", "var")),
        P("parts"),
        P(),
        P(None, None, "patch"),
        P("patch", None),
        P(),
        P(None, None, "patch"),
        P("patch", None),
    )
    out_specs = P("patch", ("parts", "var"), None)
    return jax.shard_map(
        functools.partial(on_device, mesh.shape["patch"], mesh.shape["var"]),
        mesh=mesh, in_specs=in_specs, out_specs=out_specs, check_vma=False,
    )
```

```python
import functools

import jax
import jax.numpy as jnp
from jax import lax
from jax.experimental import pallas as pl
from jax.experimental.pallas import tpu as pltpu
from jax.sharding import PartitionSpec as P

HD = 64
REACH = 5
EPS = 1e-06
MESH = pl.DeviceIdType.MESH
F32 = jnp.float32
BF16 = jnp.bfloat16


def norm_rows(rows, gain):
    floats = rows.astype(F32)
    scaled = floats * lax.rsqrt(jnp.mean(floats * floats, axis=-1, keepdims=True) + EPS)
    return (scaled * gain).astype(BF16)


def dot(a, b):
    return jnp.dot(a, b, preferred_element_type=F32)


def dot_t(a, b):
    return lax.dot_general(a, b, (((1,), (1,)), ((), ())), preferred_element_type=F32)


def kernel(
    n, nvar, tok, marks, gids, tgain, sgain, wt_in, wot_in, wqs_in, wos_in,
    out, gx, mk, wt, wot, wqs, wos, att, ratt, mid, sw, kvb, qb, prod, sc, pb,
    local_sem, tok_s, tok_r, mk_s, mk_r, w_s, w_r, att_s, att_r, win_s, win_r,
):
    me = lax.axis_index("patch")
    var = lax.axis_index("var")
    nv, pp, dm = tok.shape
    hw = wot_in.shape[0]
    heads = hw // HD
    side = (me + 1 - 2 * (me % 2), me + 2 - 4 * ((me // 2) % 2), n - 1 - me)
    sib = var + 1 - 2 * (var % 2)
    core = var % 2
    nbrs = (1, -1, 2, -2)

    def exists(k):
        return (var + k >= 0) & (var + k < nvar)

    barrier = pltpu.get_barrier_semaphore()
    count = n - 1 + 1
    for other in side:
        pl.semaphore_signal(barrier, inc=1, device_id={"patch": other}, device_id_type=MESH)
    pl.semaphore_signal(barrier, inc=1, device_id={"var": sib}, device_id_type=MESH)
    for k in nbrs:
        @pl.when(exists(k))
        def _():
            pl.semaphore_signal(barrier, inc=1, device_id={"var": var + k}, device_id_type=MESH)
        count = count + exists(k).astype(jnp.int32)
    own = [
        pltpu.make_async_copy(wot_in, wot.at[me], local_sem.at[0]),
        pltpu.make_async_copy(wqs_in, wqs.at[me], local_sem.at[1]),
        pltpu.make_async_copy(wos_in, wos.at[me], local_sem.at[2]),
        pltpu.make_async_copy(wt_in, wt, local_sem.at[3]),
        pltpu.make_async_copy(tok, gx.at[:, pl.ds(pl.multiple_of(me * pp, pp), pp), :], local_sem.at[4]),
    ]
    for i in (4, 3, 0, 1, 2):
        own[i].start()
    pl.semaphore_wait(barrier, count)

    sends = []

    def remote(src, dst, ssem, rsem, **where):
        c = pltpu.make_async_remote_copy(
            src_ref=src, dst_ref=dst, send_sem=ssem, recv_sem=rsem, device_id=where, device_id_type=MESH
        )
        return c

    def launch(*a, **k):
        c = remote(*a, **k)
        c.start()
        sends.append(c)
        return c

    def block(of, lo=0, num=pp):
        return pl.ds(pl.multiple_of(of * pp + lo, num), num)

    half = pp // 2
    mk_c = [launch(marks, mk.at[me], mk_s.at[d], mk_r.at[d], patch=side[d]) for d in range(3)]
    tok_c = {}
    for i in range(nv):
        for d in (0, 1):
            v = i if d == 1 else nv - 1 - i
            tok_c[d, v] = launch(tok.at[v], gx.at[v, block(me), :], tok_s.at[d, v], tok_r.at[d, v], patch=side[d])
    routes = ((1, 0, 0, pp), (0, 2, 0, pp), (1, 1, 0, half), (0, 1, half, half))
    diag_c = []
    for i, (d, v, lo, num) in enumerate(routes):
        tok_c[d, v].wait_recv()
        piece = gx.at[v, block(side[d], lo, num), :]
        diag_c.append(launch(piece, piece, tok_s.at[2, i], tok_r.at[2, i], patch=side[1 - d]))

    arrays = ((wot_in, wot), (wqs_in, wqs), (wos_in, wos))
    wc = {}

    def piece_of(a, shard, part=None):
        rows = arrays[a][1].shape[1] // 2
        if part is None:
            return arrays[a][1].at[shard, pl.ds(pl.multiple_of(core * rows, rows), rows), :]
        num = rows // 2
        return arrays[a][1].at[shard, pl.ds(pl.multiple_of(core * rows + part * num, num), num), :]

    def w_own(a):
        src = arrays[a][0]
        rows = src.shape[0] // 2
        for d in (0, 1):
            wc[a, d] = launch(
                src.at[pl.ds(pl.multiple_of(core * rows, rows), rows), :], piece_of(a, me),
                w_s.at[a, d], w_r.at[a, d], patch=side[d],
            )

    def w_relay(a):
        for d in (0, 1):
            wc[a, d].wait_recv()
            piece = piece_of(a, side[d], 1 - d)
            wc[a, 2 + d] = launch(piece, piece, w_s.at[a, 2 + d], w_r.at[a, 2 + d], patch=side[1 - d])
            piece = piece_of(a, side[d])
            wc[a, 4 + d] = launch(piece, piece, w_s.at[a, 4 + d], w_r.at[a, 4 + d], var=sib)

    def w_diag(a):
        wc[a, 2].wait_recv()
        wc[a, 3].wait_recv()
        piece = piece_of(a, side[2])
        wc[a, 6] = launch(piece, piece, w_s.at[a, 6], w_r.at[a, 6], var=sib)

    w_own(0)
    w_own(2)
    for k in nbrs:
        lo = {1: 9, -1: 3, 2: 12, -2: 1}[k]
        num = nv if abs(k) == 1 else nv - 1

        @pl.when(jnp.logical_not(exists(k)))
        def _():
            sw[lo:lo + num] = jnp.zeros((num, pp, dm), BF16)

    mk[me] = marks[...]
    own[3].wait()
    own[4].wait()
    for c in mk_c:
        c.wait_recv()
    for d in (0, 1):
        for v in range(nv):
            if (d, v) not in [r[:2] for r in routes]:
                tok_c[d, v].wait_recv()
    for c in diag_c:
        c.wait_recv()

    full = n * pp
    seen = jnp.concatenate([mk[s] for s in range(n)], axis=1)
    qi = lax.broadcasted_iota(jnp.int32, (full, full), 0)
    ki = lax.broadcasted_iota(jnp.int32, (full, full), 1)
    att_c = []
    for v in range(nv):
        normed = norm_rows(gx[v], tgain[...])
        proj = dot_t(normed, wt[...]).astype(BF16)
        allowed = ((ki < qi) & (seen[v:v + 1, :] > 0)) | (ki == qi)
        outs = []
        for h in range(heads):
            q = proj[:, h * HD:(h + 1) * HD]
            k = proj[:, hw + h * HD:hw + (h + 1) * HD]
            val = proj[:, 2 * hw + h * HD:2 * hw + (h + 1) * HD]
            s = lax.dot_general(q, k, (((1,), (1,)), ((), ())), preferred_element_type=F32) * HD ** (-0.5)
            s = jnp.where(allowed, s, -jnp.inf)
            e = jnp.exp(s - jnp.max(s, axis=-1, keepdims=True))
            w = (e / jnp.sum(e, axis=-1, keepdims=True)).astype(BF16)
            outs.append(dot(w, val).astype(BF16))
        att[v] = jnp.concatenate(outs, axis=1)
        for d in (2, 0, 1):
            att_c.append(launch(att.at[v, block(side[d]), :], ratt.at[me, v], att_s.at[v, d], att_r.at[v, d], patch=side[d]))
        ratt[me, v] = att[v, block(me), :]
    w_relay(0)
    w_own(1)
    own[0].wait()
    for c in att_c:
        c.wait_recv()
    w_diag(0)
    for k in (4, 5, 6):
        wc[0, k].wait_recv()

    rows = nv * pp
    mix = jnp.zeros((rows, dm), F32)
    for s in range(n):
        mix = mix + dot(ratt[s].reshape(rows, hw), wot[s]).astype(BF16).astype(F32)
    middle = (gx[:, block(me), :].reshape(rows, dm).astype(F32) + mix).astype(BF16)
    mid[...] = middle
    sw[6:6 + nv] = norm_rows(middle, sgain[...]).reshape(nv, pp, dm)

    def window(k, i):
        src = {1: (6, 9), -1: (6, 9), 2: (7, 9), -2: (6, 8)}[k]
        dst = {1: (3, 6), -1: (9, 12), 2: (1, 3), -2: (12, 14)}[k]
        return remote(sw.at[src[0]:src[1]], sw.at[dst[0]:dst[1]], win_s.at[i], win_r.at[i], var=var + k)

    for i, k in enumerate(nbrs):
        @pl.when(exists(k))
        def _():
            window(k, i).start()

    own[1].wait()
    own[2].wait()
    w_relay(1)
    w_relay(2)
    for i, k in enumerate(nbrs):
        @pl.when(exists(-k))
        def _():
            window(k, i).wait_recv()

    nkey = 4 + 3 * nv
    pairs = [(u, u + 6 + t) for u in range(nv) for t in range(-REACH, REACH + 1)]
    sc[...] = jnp.zeros_like(sc)

    def scores_of(s):
        qb[...] = dot_t(sw[6:6 + nv].reshape(rows, dm), wqs[s, :hw, :]).astype(BF16).reshape(nv, pp, hw)
        kvb[s] = dot_t(sw[1:1 + nkey].reshape(nkey * pp, dm), wqs[s, hw:, :]).astype(BF16).reshape(nkey, pp, 2 * hw)
        for i, (u, j) in enumerate(pairs):
            prod[i * pp:(i + 1) * pp, :] = (
                qb[u].astype(F32) * kvb[s, j - 1, :, :hw].astype(F32)
            ).astype(BF16)
        lane = lax.broadcasted_iota(jnp.int32, (hw, 128), 0) // HD + heads * s
        col = lax.broadcasted_iota(jnp.int32, (hw, 128), 1)
        sc[...] += dot(prod[...], (lane == col).astype(F32).astype(BF16))

    def soften():
        total = gids.shape[0]
        local_n = total // nv
        base = (var % local_n) * nv
        for u in range(nv):
            mine_group = gids[base + u]
            slabs = []
            for t in range(-REACH, REACH + 1):
                w = base + u + t
                inside = (w >= 0) & (w < total)
                at = jnp.minimum(jnp.maximum(w, 0), total - 1)
                i = pairs.index((u, u + 6 + t))
                ok = inside & (gids[at] == mine_group)
                slabs.append(jnp.where(ok, sc[i * pp:(i + 1) * pp, :] * HD ** (-0.5), -jnp.inf))
            top = functools.reduce(jnp.maximum, slabs)
            es = [jnp.exp(x - top) for x in slabs]
            den = functools.reduce(lambda a, b: a + b, es)
            for t, e in enumerate(es):
                i = u * (2 * REACH + 1) + t
                pb[i * pp:(i + 1) * pp, :] = (e / den).astype(BF16)

    def mix_of(s):
        lane = lax.broadcasted_iota(jnp.int32, (128, hw), 1) // HD + heads * s
        col = lax.broadcasted_iota(jnp.int32, (128, hw), 0)
        spread = (lane == col).astype(F32).astype(BF16)
        done = []
        for u in range(nv):
            total_u = jnp.zeros((pp, hw), F32)
            lo = u * (2 * REACH + 1)
            wide = dot(pb[lo * pp:(lo + 2 * REACH + 1) * pp, :], spread)
            for t in range(2 * REACH + 1):
                val = kvb[s, u + t, :, hw:].astype(F32)
                total_u = total_u + wide[t * pp:(t + 1) * pp] * val
            done.append(total_u.astype(BF16))
        res = dot(jnp.concatenate(done, axis=0), wos[s]).astype(BF16).astype(F32)
        return res

    scores_of(me)
    for d in (0, 1):
        wc[1, 4 + d].wait_recv()
        scores_of(side[d])
    w_diag(1)
    soften()
    mix2 = mix_of(me)
    for d in (0, 1):
        wc[2, 4 + d].wait_recv()
        mix2 = mix2 + mix_of(side[d])
    w_diag(2)
    wc[1, 6].wait_recv()
    scores_of(side[2])
    soften()
    wc[2, 6].wait_recv()
    mix2 = mix2 + mix_of(side[2])
    out[...] = (mid[...].astype(F32) + mix2).astype(BF16).reshape(nv, pp, dm)

    for c in sends:
        c.wait_send()
    for i, k in enumerate(nbrs):
        @pl.when(exists(k))
        def _():
            window(k, i).wait_send()


def on_device(n, nvar, tokens, patch_mask, group_ids, time_gain, time_qkv, time_out, space_gain, space_qkv, space_out):
    pp, nv, dm = tokens.shape
    hw = time_out.shape[0]
    tok = jnp.transpose(tokens, (1, 0, 2))
    wt = jnp.transpose(time_qkv, (1, 2, 0)).reshape(3 * hw, dm)
    wqs = jnp.transpose(space_qkv, (1, 2, 0)).reshape(3 * hw, dm)
    npair = nv * (2 * REACH + 1)
    vm = pl.BlockSpec(memory_space=pltpu.VMEM)
    anyv = pl.BlockSpec(memory_space=pltpu.HBM)
    dma = pltpu.SemaphoreType.DMA
    res = pl.pallas_call(
        functools.partial(kernel, n, nvar),
        out_shape=jax.ShapeDtypeStruct((nv, pp, dm), BF16),
        in_specs=[anyv, vm, pl.BlockSpec(memory_space=pltpu.SMEM), vm, vm, anyv, anyv, anyv, anyv],
        out_specs=vm,
        scratch_shapes=[
            pltpu.VMEM((nv, n * pp, dm), BF16),
            pltpu.VMEM((n, nv, pp), jnp.int32),
            pltpu.VMEM((3 * hw, dm), BF16),
            pltpu.VMEM((n, hw, dm), BF16),
            pltpu.VMEM((n, 3 * hw, dm), BF16),
            pltpu.VMEM((n, hw, dm), BF16),
            pltpu.VMEM((nv, n * pp, hw), BF16),
            pltpu.VMEM((n, nv, pp, hw), BF16),
            pltpu.VMEM((nv * pp, dm), BF16),
            pltpu.VMEM((5 * nv, pp, dm), BF16),
            pltpu.VMEM((n, 4 + 3 * nv, pp, 2 * hw), BF16),
            pltpu.VMEM((nv, pp, hw), BF16),
            pltpu.VMEM((npair * pp, hw), BF16),
            pltpu.VMEM((npair * pp, 128), F32),
            pltpu.VMEM((npair * pp, 128), BF16),
            dma((5,)), dma((3, 4)), dma((3, 4)), dma((3,)), dma((3,)),
            dma((3, 7)), dma((3, 7)), dma((nv, 3)), dma((nv, 3)), dma((4,)), dma((4,)),
        ],
        compiler_params=pltpu.CompilerParams(
            collective_id=0, has_side_effects=True, vmem_limit_bytes=67_000_000
        ),
    )(tok, patch_mask.T, group_ids, time_gain, space_gain, wt, time_out, wqs, space_out)
    return jnp.transpose(res, (1, 0, 2))


def solution(mesh):
    in_specs = (
        P("patch", ("parts", "var"), None),
        P("patch", ("parts", "var")),
        P("parts"),
        P(),
        P(None, None, "patch"),
        P("patch", None),
        P(),
        P(None, None, "patch"),
        P("patch", None),
    )
    out_specs = P("patch", ("parts", "var"), None)
    return jax.shard_map(
        functools.partial(on_device, mesh.shape["patch"], mesh.shape["var"]),
        mesh=mesh, in_specs=in_specs, out_specs=out_specs, check_vma=False,
    )
```
